32 devices in a mesh: dp: 8 (over z, x), owner: 4 (over y, core).
Axes of the slice: x: 2, y: 2, z: 4, core: 2. Of those that a mesh axis runs over, the one named last changes fastest.
Arguments:
- gradients: float32 [8, 1024, 7168], P(None, 'dp', 'owner'), may hold values from -6 to 6
- rows_live: int32 [8], replicated, may hold values from 256 to 1024
Outputs:
- updates: bfloat16 [8, 1024, 7168], P(None, 'dp', 'owner')
The draws below stay inside these ranges and needn't reach their ends.
All inputs are finite; a program needn't handle non-finite values.
Results may differ from the reference program's by a relative error of at most 0.015.
Values may be sent and summed in bfloat16 or wider, within the bound.
A program may use at most 64 MiB of HBM per device.

```python
import math
import jax
import jax.numpy as jnp
from jax import lax

D = 7168
FF_WIN = 1024
MATRICES = 8
N_OWNER = 4


def with_ends(values, stream_key, smallest, top_value):
    shape = values.shape
    spot = [jax.random.randint(jax.random.fold_in(stream_key, axis), (), 0, shape[axis]) for axis in range(len(shape))]
    values = values.at[tuple(spot)].set(smallest)
    longest = shape.index(max(shape))
    spot[longest] = (spot[longest] + 1) % shape[longest]
    return values.at[tuple(spot)].set(top_value)


def shard_levels(key, dims, cuts, smallest, top_value):
    factor_of, own = 1.0, jax.random.fold_in(key, 6)
    for dim, parts in cuts:
        steps = jnp.exp(jax.random.uniform(jax.random.fold_in(own, dim), (parts,), jnp.float32, smallest / len(cuts), top_value / len(cuts)))
        factor_of = factor_of * jnp.repeat(steps, dims[dim] // parts).reshape([-1 if axis == dim else 1 for axis in range(len(dims))])
    return factor_of


def scatter_about(stream_key, shape, deviation, bound, pieces=(), kind=jnp.bfloat16):
    array = deviation * jax.random.normal(stream_key, shape, jnp.float32)
    if pieces:
        array = array * shard_levels(stream_key, shape, pieces, -0.22, 0.18)
    return jnp.clip(array, -bound, bound).astype(kind)


def setup_inputs(seed: int = 0) -> dict:
    arg_keys = jax.random.split(jax.random.key(seed), 3)
    gradients = scatter_about(arg_keys[0], (MATRICES, FF_WIN, D), 1.0, 6.0, ((1, 8), (2, 4)), jnp.float32)
    rows_live = with_ends(jax.random.randint(arg_keys[1], (MATRICES,), FF_WIN // 4, FF_WIN + 1), jax.random.fold_in(arg_keys[1], 1), FF_WIN // 4, FF_WIN).astype(jnp.int32)
    return dict(gradients=gradients, rows_live=rows_live)


def one_matrix(packed):
    gradient, live_count = packed
    narrow = gradient.astype(jnp.bfloat16)
    live_mask = jnp.arange(FF_WIN, dtype=jnp.int32)[:, None] < live_count
    narrow = jnp.where(live_mask, narrow, jnp.zeros_like(narrow))
    width = D // N_OWNER
    blocks = narrow.reshape(FF_WIN, N_OWNER, width).transpose(1, 0, 2)

    def add_block(total, block):
        term = jnp.dot(block, block.T, preferred_element_type=jnp.float32)
        rounded = lax.optimization_barrier(term.astype(jnp.bfloat16))
        return (total + rounded.astype(jnp.float32), None)
    gram, unused = lax.scan(add_block, jnp.zeros((FF_WIN, FF_WIN), jnp.float32), blocks)
    scale_sq = 2.0 * jnp.trace(gram) / live_count.astype(jnp.float32)
    inverse = 1.0 / jnp.sqrt(scale_sq)
    normed_gram = (gram / scale_sq).astype(jnp.bfloat16)
    once = jnp.dot(normed_gram, narrow, preferred_element_type=jnp.float32) * inverse
    twice = jnp.dot(normed_gram, once.astype(jnp.bfloat16), preferred_element_type=jnp.float32)
    result = 3.4445 * narrow.astype(jnp.float32) * inverse - 4.775 * once + 2.0315 * twice
    return (result * (0.2 * math.sqrt(D))).astype(jnp.bfloat16)

def reference(gradients, rows_live):
    return lax.map(one_matrix, (gradients, rows_live))
```

```python
import functools
import math

import jax
import jax.numpy as jnp
from jax import lax
from jax.experimental import pallas as pl
from jax.experimental.pallas import tpu as pltpu
from jax.sharding import PartitionSpec as P

MESH = pl.DeviceIdType.MESH
NT = (((1,), (1,)), ((), ()))
NN = (((1,), (0,)), ((), ()))


def flip(index, bits, count):
    out, bit = 0, 1
    while bit < count:
        out = out + bit * (((index // bit) % 2 + (bits // bit) % 2) % 2)
        bit *= 2
    return out


def kernel(
    n, owners, width_all, live_ref, grad_ref, out_ref,
    stage, send, rows, gram, normed, upd, part, got,
    load_sem, send_sem, recv_sem, psend_sem, precv_sem, usend_sem, urecv_sem, own_sem,
):
    d = lax.axis_index("dp")
    o = lax.axis_index("owner")
    size, width = stage.shape[1], stage.shape[2]
    hidden = rows.shape[0]
    strip = max(size, min(128, hidden))
    strips = hidden // strip
    per = strip // size
    levels = owners.bit_length() - 1

    def far_first(j):
        return 1 + (j + n // 2 - 1) % (n - 1)

    def load(slot):
        return pltpu.make_async_copy(grad_ref.at[flip(d, slot, n)], stage.at[slot], load_sem.at[slot])

    def forward(slot):
        return pltpu.make_async_remote_copy(
            src_ref=send.at[slot],
            dst_ref=rows.at[pl.ds(pl.multiple_of(slot * size, size), size)],
            send_sem=send_sem.at[slot],
            recv_sem=recv_sem.at[slot],
            device_id={"dp": flip(d, slot, n)},
            device_id_type=MESH,
        )

    def back(slot):
        return pltpu.make_async_remote_copy(
            src_ref=upd.at[pl.ds(pl.multiple_of(slot * size, size), size)],
            dst_ref=out_ref.at[d],
            send_sem=usend_sem.at[slot],
            recv_sem=urecv_sem.at[slot],
            device_id={"dp": flip(d, slot, n)},
            device_id_type=MESH,
        )

    def back_arrival(slot):
        return pltpu.make_async_remote_copy(
            src_ref=upd.at[pl.ds(pl.multiple_of(slot * size, size), size)],
            dst_ref=out_ref.at[flip(d, slot, n)],
            send_sem=usend_sem.at[slot],
            recv_sem=urecv_sem.at[slot],
            device_id={"dp": flip(d, slot, n)},
            device_id_type=MESH,
        )

    def share(level, s):
        cols = (s + 1) * strip
        return pltpu.make_async_remote_copy(
            src_ref=part.at[level, s, :, pl.ds(0, cols)],
            dst_ref=got.at[level, s, :, pl.ds(0, cols)],
            send_sem=psend_sem.at[level, s],
            recv_sem=precv_sem.at[level, s],
            device_id={"owner": flip(o, 2**level, owners)},
            device_id_type=MESH,
        )

    @pl.loop(0, n - 1)
    def _(j):
        load(far_first(j)).start()

    load(0).start()

    barrier = pltpu.get_barrier_semaphore()

    @pl.loop(1, n)
    def _(k):
        pl.semaphore_signal(barrier, inc=1, device_id={"dp": flip(d, k, n)}, device_id_type=MESH)

    for level in range(levels):
        pl.semaphore_signal(
            barrier, inc=1, device_id={"owner": flip(o, 2**level, owners)}, device_id_type=MESH
        )
    pl.semaphore_wait(barrier, n - 1 + levels)

    row_index = d * size + lax.broadcasted_iota(jnp.int32, (size, width), 0)

    def narrow(slot):
        load(slot).wait()
        live = live_ref[flip(d, slot, n)]
        return jnp.where(row_index < live, stage[slot], 0.0).astype(jnp.bfloat16)

    @pl.loop(0, n - 1)
    def _(j):
        slot = far_first(j)
        send[slot] = narrow(slot)
        forward(slot).start()

    rows[pl.ds(0, size), :] = narrow(0)

    eye = (
        lax.broadcasted_iota(jnp.int32, (strip, strip), 0)
        == lax.broadcasted_iota(jnp.int32, (strip, strip), 1)
    )
    trace = jnp.zeros((1, 1), jnp.float32)

    def settle(s, trace):
        at = s * strip
        cols = at + strip
        share(levels - 1, s).wait_recv()
        total = (
            part[levels - 1, s, :, 0:cols].astype(jnp.float32)
            + got[levels - 1, s, :, 0:cols].astype(jnp.float32)
        )
        gram[at:cols, 0:cols] = total
        for j in range(s):
            gram[j * strip : (j + 1) * strip, at:cols] = total[:, j * strip : (j + 1) * strip].T
        own = jnp.where(eye, total[:, at:cols], 0.0)
        return trace + jnp.sum(own, keepdims=True)

    for s in range(strips):
        cols = (s + 1) * strip
        if s == 0:
            @pl.loop(1, per)
            def _(k):
                forward(k).wait_recv()
        else:
            @pl.loop(s * per, (s + 1) * per)
            def _(k):
                forward(k).wait_recv()

        part[0, s, :, 0:cols] = lax.dot_general(
            rows[s * strip : cols, :], rows[0:cols, :], NT, preferred_element_type=jnp.float32
        ).astype(jnp.bfloat16)
        share(0, s).start()
        if s > 0:
            trace = settle(s - 1, trace)
        for level in range(1, levels):
            share(level - 1, s).wait_recv()
            part[level, s, :, 0:cols] = (
                part[level - 1, s, :, 0:cols].astype(jnp.float32)
                + got[level - 1, s, :, 0:cols].astype(jnp.float32)
            ).astype(jnp.bfloat16)
            share(level, s).start()
    trace = settle(strips - 1, trace)

    live_count = jnp.full((1, 1), live_ref[d], jnp.int32).astype(jnp.float32)
    scale_sq = 2.0 * trace / live_count
    shrink = 1.0 / scale_sq
    gain = (0.2 * math.sqrt(width_all)) / jnp.sqrt(scale_sq)

    @pl.loop(0, strips)
    def _(s):
        at = pl.ds(pl.multiple_of(s * strip, strip), strip)
        normed[at, :] = (gram[at, :] * shrink).astype(jnp.bfloat16)

    def update(s):
        at = pl.ds(pl.multiple_of(s * strip, strip), strip)
        square = lax.dot_general(normed[at, :], normed[...], NN, preferred_element_type=jnp.float32)
        mix = (2.0315 * square - 4.775 * normed[at, :].astype(jnp.float32)).astype(jnp.bfloat16)
        moved = lax.dot_general(mix, rows[...], NN, preferred_element_type=jnp.float32)
        upd[at, :] = ((3.4445 * rows[at, :].astype(jnp.float32) + moved) * gain).astype(jnp.bfloat16)

    if per == 1:
        @pl.loop(0, n - 1)
        def _(j):
            slot = far_first(j)
            update(slot)
            back(slot).start()

        update(0)
    else:
        @pl.loop(1, strips)
        def _(s):
            update(s)

            @pl.loop(0, per)
            def _(k):
                back(s * per + k).start()

        update(0)

        @pl.loop(1, per)
        def _(k):
            back(k).start()

    own_copy = pltpu.make_async_copy(upd.at[pl.ds(0, size)], out_ref.at[d], own_sem)
    own_copy.start()

    for s in range(strips):
        for level in range(levels):
            share(level, s).wait_send()

    @pl.loop(1, n)
    def _(k):
        forward(k).wait_send()

    @pl.loop(1, n)
    def _(k):
        back(k).wait_send()
        back_arrival(k).wait_recv()

    own_copy.wait()


def solution(mesh):
    n, owners = mesh.shape["dp"], mesh.shape["owner"]

    def body(gradients, rows_live):
        matrices, size, width = gradients.shape
        hidden = size * n
        strip = max(size, min(128, hidden))
        strips = hidden // strip
        levels = owners.bit_length() - 1
        dma = pltpu.SemaphoreType.DMA
        return pl.pallas_call(
            functools.partial(kernel, n, owners, width * owners),
            out_shape=jax.ShapeDtypeStruct((matrices, size, width), jnp.bfloat16),
            in_specs=[
                pl.BlockSpec(memory_space=pltpu.SMEM),
                pl.BlockSpec(memory_space=pl.ANY),
            ],
            out_specs=pl.BlockSpec(memory_space=pl.ANY),
            scratch_shapes=[
                pltpu.VMEM((n, size, width), jnp.float32),
                pltpu.VMEM((n, size, width), jnp.bfloat16),
                pltpu.VMEM((hidden, width), jnp.bfloat16),
                pltpu.VMEM((hidden, hidden), jnp.float32),
                pltpu.VMEM((hidden, hidden), jnp.bfloat16),
                pltpu.VMEM((hidden, width), jnp.bfloat16),
                pltpu.VMEM((levels, strips, strip, hidden), jnp.bfloat16),
                pltpu.VMEM((levels, strips, strip, hidden), jnp.bfloat16),
                dma((n,)), dma((n,)), dma((n,)),
                dma((levels, strips)), dma((levels, strips)),
                dma((n,)), dma((n,)), dma,
            ],
            compiler_params=pltpu.CompilerParams(
                collective_id=0, has_side_effects=True, vmem_limit_bytes=60 * 2**20
            ),
        )(rows_live, gradients)

    return jax.shard_map(
        body,
        mesh=mesh,
        in_specs=(P(None, "dp", "owner"), P()),
        out_specs=P(None, "dp", "owner"),
        check_vma=False,
    )
```

```python
import functools
import math

import jax
import jax.numpy as jnp
from jax import lax
from jax.experimental import pallas as pl
from jax.experimental.pallas import tpu as pltpu
from jax.sharding import PartitionSpec as P

MESH = pl.DeviceIdType.MESH
NT = (((1,), (1,)), ((), ()))
NN = (((1,), (0,)), ((), ()))


def flip(index, bits, count):
    out, bit = 0, 1
    while bit < count:
        out = out + bit * (((index // bit) % 2 + (bits // bit) % 2) % 2)
        bit *= 2
    return out


def kernel(
    n, owners, width_all, live_ref, grad_ref, out_ref,
    stage, send, rows, gram, normed, upd, part, got,
    load_sem, send_sem, recv_sem, psend_sem, precv_sem, usend_sem, urecv_sem, own_sem,
):
    d = lax.axis_index("dp")
    o = lax.axis_index("owner")
    size, width = stage.shape[1], stage.shape[2]
    hidden = rows.shape[0]
    strip = max(size, min(128, hidden))
    strips = hidden // strip
    per = strip // size
    levels = owners.bit_length() - 1

    inner = ((d // (n // 2)) % 2 + (d // (n // 4)) % 2) % 2
    to_inner = n // 2 + inner * (n // 4)
    to_outer = n // 2 + (1 - inner) * (n // 4)

    def each(start, count):
        def over(fn):
            @pl.loop(0, count)
            def _(j):
                fn(start + j)
        return over

    def gather_order(fn):
        each(to_inner, n // 4)(fn)
        each(1, n // 2 - 1)(fn)
        each(to_outer, n // 4)(fn)

    def return_order(fn):
        each(to_outer, n // 4)(fn)
        each(to_inner, n // 4)(fn)
        each(1, n // 2 - 1)(fn)

    def load(slot):
        return pltpu.make_async_copy(grad_ref.at[flip(d, slot, n)], stage.at[slot], load_sem.at[slot])

    def forward(slot):
        return pltpu.make_async_remote_copy(
            src_ref=send.at[slot],
            dst_ref=rows.at[pl.ds(pl.multiple_of(slot * size, size), size)],
            send_sem=send_sem.at[slot],
            recv_sem=recv_sem.at[slot],
            device_id={"dp": flip(d, slot, n)},
            device_id_type=MESH,
        )

    def back(slot):
        return pltpu.make_async_remote_copy(
            src_ref=upd.at[pl.ds(pl.multiple_of(slot * size, size), size)],
            dst_ref=out_ref.at[d],
            send_sem=usend_sem.at[slot],
            recv_sem=urecv_sem.at[slot],
            device_id={"dp": flip(d, slot, n)},
            device_id_type=MESH,
        )

    def back_arrival(slot):
        return pltpu.make_async_remote_copy(
            src_ref=upd.at[pl.ds(pl.multiple_of(slot * size, size), size)],
            dst_ref=out_ref.at[flip(d, slot, n)],
            send_sem=usend_sem.at[slot],
            recv_sem=urecv_sem.at[slot],
            device_id={"dp": flip(d, slot, n)},
            device_id_type=MESH,
        )

    def share(level, s):
        cols = (s + 1) * strip
        return pltpu.make_async_remote_copy(
            src_ref=part.at[level, s, :, pl.ds(0, cols)],
            dst_ref=got.at[level, s, :, pl.ds(0, cols)],
            send_sem=psend_sem.at[level, s],
            recv_sem=precv_sem.at[level, s],
            device_id={"owner": flip(o, 2**level, owners)},
            device_id_type=MESH,
        )

    gather_order(lambda slot: load(slot).start())
    load(0).start()

    barrier = pltpu.get_barrier_semaphore()

    @pl.loop(1, n)
    def _(k):
        pl.semaphore_signal(barrier, inc=1, device_id={"dp": flip(d, k, n)}, device_id_type=MESH)

    for level in range(levels):
        pl.semaphore_signal(
            barrier, inc=1, device_id={"owner": flip(o, 2**level, owners)}, device_id_type=MESH
        )
    pl.semaphore_wait(barrier, n - 1 + levels)

    row_index = d * size + lax.broadcasted_iota(jnp.int32, (size, width), 0)

    def narrow(slot):
        load(slot).wait()
        live = live_ref[flip(d, slot, n)]
        return jnp.where(row_index < live, stage[slot], 0.0).astype(jnp.bfloat16)

    @gather_order
    def _(slot):
        send[slot] = narrow(slot)
        forward(slot).start()

    rows[pl.ds(0, size), :] = narrow(0)

    eye = (
        lax.broadcasted_iota(jnp.int32, (strip, strip), 0)
        == lax.broadcasted_iota(jnp.int32, (strip, strip), 1)
    )
    trace = jnp.zeros((1, 1), jnp.float32)

    def settle(s, trace):
        at = s * strip
        cols = at + strip
        share(levels - 1, s).wait_recv()
        total = (
            part[levels - 1, s, :, 0:cols].astype(jnp.float32)
            + got[levels - 1, s, :, 0:cols].astype(jnp.float32)
        )
        gram[at:cols, 0:cols] = total
        for j in range(s):
            gram[j * strip : (j + 1) * strip, at:cols] = total[:, j * strip : (j + 1) * strip].T
        own = jnp.where(eye, total[:, at:cols], 0.0)
        return trace + jnp.sum(own, keepdims=True)

    for s in range(strips):
        cols = (s + 1) * strip
        if s == 0:
            @pl.loop(1, per)
            def _(k):
                forward(k).wait_recv()
        else:
            @pl.loop(s * per, (s + 1) * per)
            def _(k):
                forward(k).wait_recv()

        part[0, s, :, 0:cols] = lax.dot_general(
            rows[s * strip : cols, :], rows[0:cols, :], NT, preferred_element_type=jnp.float32
        ).astype(jnp.bfloat16)
        share(0, s).start()
        if s > 1:
            trace = settle(s - 2, trace)
        for level in range(1, levels):
            share(level - 1, s).wait_recv()
            part[level, s, :, 0:cols] = (
                part[level - 1, s, :, 0:cols].astype(jnp.float32)
                + got[level - 1, s, :, 0:cols].astype(jnp.float32)
            ).astype(jnp.bfloat16)
            share(level, s).start()
    for s in range(max(strips - 2, 0), strips):
        trace = settle(s, trace)

    live_count = jnp.full((1, 1), live_ref[d], jnp.int32).astype(jnp.float32)
    scale_sq = 2.0 * trace / live_count
    shrink = 1.0 / scale_sq
    gain = (0.2 * math.sqrt(width_all)) / jnp.sqrt(scale_sq)

    @pl.loop(0, strips)
    def _(s):
        at = pl.ds(pl.multiple_of(s * strip, strip), strip)
        normed[at, :] = (gram[at, :] * shrink).astype(jnp.bfloat16)

    def update(s):
        at = pl.ds(pl.multiple_of(s * strip, strip), strip)
        square = lax.dot_general(normed[at, :], normed[...], NN, preferred_element_type=jnp.float32)
        mix = (2.0315 * square - 4.775 * normed[at, :].astype(jnp.float32)).astype(jnp.bfloat16)
        moved = lax.dot_general(mix, rows[...], NN, preferred_element_type=jnp.float32)
        upd[at, :] = ((3.4445 * rows[at, :].astype(jnp.float32) + moved) * gain).astype(jnp.bfloat16)

    if per == 1:
        @return_order
        def _(slot):
            update(slot)
            back(slot).start()

        update(0)
    else:
        @pl.loop(1, strips)
        def _(s):
            update(s)

            @pl.loop(0, per)
            def _(k):
                back(s * per + k).start()

        update(0)

        @pl.loop(1, per)
        def _(k):
            back(k).start()

    own_copy = pltpu.make_async_copy(upd.at[pl.ds(0, size)], out_ref.at[d], own_sem)
    own_copy.start()

    for s in range(strips):
        for level in range(levels):
            share(level, s).wait_send()

    @pl.loop(1, n)
    def _(k):
        forward(k).wait_send()

    @pl.loop(1, n)
    def _(k):
        back(k).wait_send()
        back_arrival(k).wait_recv()

    own_copy.wait()


def solution(mesh):
    n, owners = mesh.shape["dp"], mesh.shape["owner"]

    def body(gradients, rows_live):
        matrices, size, width = gradients.shape
        hidden = size * n
        strip = max(size, min(128, hidden))
        strips = hidden // strip
        levels = owners.bit_length() - 1
        dma = pltpu.SemaphoreType.DMA
        return pl.pallas_call(
            functools.partial(kernel, n, owners, width * owners),
            out_shape=jax.ShapeDtypeStruct((matrices, size, width), jnp.bfloat16),
            in_specs=[
                pl.BlockSpec(memory_space=pltpu.SMEM),
                pl.BlockSpec(memory_space=pl.ANY),
            ],
            out_specs=pl.BlockSpec(memory_space=pl.ANY),
            scratch_shapes=[
                pltpu.VMEM((n, size, width), jnp.float32),
                pltpu.VMEM((n, size, width), jnp.bfloat16),
                pltpu.VMEM((hidden, width), jnp.bfloat16),
                pltpu.VMEM((hidden, hidden), jnp.float32),
                pltpu.VMEM((hidden, hidden), jnp.bfloat16),
                pltpu.VMEM((hidden, width), jnp.bfloat16),
                pltpu.VMEM((levels, strips, strip, hidden), jnp.bfloat16),
                pltpu.VMEM((levels, strips, strip, hidden), jnp.bfloat16),
                dma((n,)), dma((n,)), dma((n,)),
                dma((levels, strips)), dma((levels, strips)),
                dma((n,)), dma((n,)), dma,
            ],
            compiler_params=pltpu.CompilerParams(
                collective_id=0, has_side_effects=True, vmem_limit_bytes=60 * 2**20
            ),
        )(rows_live, gradients)

    return jax.shard_map(
        body,
        mesh=mesh,
        in_specs=(P(None, "dp", "owner"), P()),
        out_specs=P(None, "dp", "owner"),
        check_vma=False,
    )
```
